16 devices in a mesh: ga: 16 (over z, y, x, core).
Axes of the slice: x: 2, y: 2, z: 2, core: 2. Of those that a mesh axis runs over, the one named last changes fastest.
Arguments:
- text_states: bfloat16 [4096, 768], P('ga')
- text_proj: bfloat16 [768, 768], replicated
- gallery: bfloat16 [32768, 768], P('ga')
- logit_scale: float32 [1], replicated
Outputs:
- output 1: bfloat16 [4096, 32768], P(None, 'ga')
- output 2: float32 [4096], replicated
All inputs are finite; a program needn't handle non-finite values.
Results may differ from the reference program's by a relative error of at most 0.001.
Values are sent between devices in bfloat16 or wider.
A program may use at most 1 GiB of HBM per device.

```python
import jax
import jax.numpy as jnp
from jax import lax

QUERIES = 4096
GALLERY = 32768
WT = 768
EMB = 768
QBLOCK = 256


def setup_inputs(seed: int = 0) -> dict:
    base_key = jax.random.key(seed)
    k_text, k_proj, k_noise, k_dirs, k_scale = jax.random.split(base_key, 5)
    text_states = jax.random.normal(k_text, (QUERIES, WT), jnp.float32)
    text_proj = jax.random.normal(k_proj, (WT, EMB), jnp.float32) * WT ** -0.5
    anchors = jax.random.normal(k_dirs, (2, EMB), jnp.float32)
    anchors = anchors / jnp.sqrt(jnp.sum(anchors * anchors, axis=1, keepdims=True))
    angles = jnp.pi * jnp.arange(GALLERY, dtype=jnp.float32) / GALLERY
    gallery = (jax.random.normal(k_noise, (GALLERY, EMB), jnp.float32) * EMB ** -0.5
               + jnp.cos(angles)[:, None] * anchors[0] + jnp.sin(angles)[:, None] * anchors[1])
    gallery = gallery / jnp.sqrt(jnp.sum(gallery * gallery, axis=1, keepdims=True))
    logit_scale = (0.5 * jnp.log(2.0 * EMB) + jnp.log(1.5)
                   + jax.random.uniform(k_scale, (1,), jnp.float32, -0.2, 0.2)).astype(jnp.float32)
    return {
        "text_states": text_states.astype(jnp.bfloat16),
        "text_proj": text_proj.astype(jnp.bfloat16),
        "gallery": gallery.astype(jnp.bfloat16),
        "logit_scale": logit_scale,
    }


def reference(text_states, text_proj, gallery, logit_scale):
    proj_out = jnp.dot(text_states, text_proj, preferred_element_type=jnp.float32)
    unit_q = proj_out / jnp.sqrt(jnp.sum(proj_out * proj_out, axis=1, keepdims=True))
    query_emb = unit_q.astype(jnp.bfloat16)
    logit_mult = jnp.exp(logit_scale[0])
    positions = jnp.arange(GALLERY, dtype=jnp.float32) / GALLERY
    blocks = query_emb.reshape(QUERIES // QBLOCK, QBLOCK, EMB)

    def score_block(query_block):
        scores = logit_mult * jnp.dot(query_block, gallery.T, preferred_element_type=jnp.float32)
        row_max = jnp.max(scores, axis=1, keepdims=True)
        exp_vals = jnp.exp(scores - row_max)
        prob_vals = exp_vals / jnp.sum(exp_vals, axis=1, keepdims=True)
        return prob_vals.astype(jnp.bfloat16), jnp.sum(prob_vals * positions, axis=1)

    prob_blocks, rank_blocks = lax.map(score_block, blocks)
    return prob_blocks.reshape(QUERIES, GALLERY), rank_blocks.reshape(QUERIES)
```

```python
import functools

import jax
import jax.numpy as jnp
from jax import lax
from jax.experimental import pallas as pl
from jax.experimental.pallas import tpu as pltpu
from jax.sharding import PartitionSpec as P

MESH = pl.DeviceIdType.MESH
LOG2E = 1.4426950408889634
F32_MAX = 3.4028234663852886e38

LEN = (96, 80, 80)
OFF = (0, 96, 176)
ROWS = 256
COLS = 2048
EMB = 768
LANES = 128
TILES = COLS // LANES


def source_mask(slot, k):
    a, b, c = 1 << k, 1 << ((k + 1) % 3), 1 << ((k + 2) % 3)
    return (0, a, b, c, a | b, a | c, b | c, 7)[slot]


def slot_of(mask, k):
    return next(s for s in range(8) if source_mask(s, k) == mask)


def relative(dev, v, h):
    out = dev
    for bit, weight in ((h, 1), (v & 1, 2), (v >> 1 & 1, 4), (v >> 2 & 1, 8)):
        if bit:
            out = out + weight * (1 - 2 * ((dev // weight) % 2))
    return out


def scale_row(t_ref):
    mult = jnp.exp(jnp.full((8, LANES), t_ref[0], jnp.float32))
    return jnp.minimum(mult * LOG2E, F32_MAX)[0:1, :]


def score_kernel(t_ref, x_hbm, w_hbm, g_hbm, e0, e1, ml0, ml1, fin_out, rank_out,
                 xv, wv, gv, q0, q1, s_acc, r_acc, cst, snd, rst, mine, fin,
                 ld_sem, pair_s, pair_r, link_s, link_r, st_s, st_r, fb_s, fb_r):
    dev = lax.axis_index("ga")
    e, ml, q = (e0, e1), (ml0, ml1), (q0, q1)

    loads = [pltpu.make_async_copy(src, dst, ld_sem.at[i])
             for i, (src, dst) in enumerate(((x_hbm, xv), (w_hbm, wv), (g_hbm, gv)))]
    for load in loads:
        load.start()
    barrier = pltpu.get_barrier_semaphore()
    for other in range(1, 16):
        pl.semaphore_signal(barrier, inc=1, device_id=(relative(dev, other >> 1, other & 1),), device_id_type=MESH)

    cc = scale_row(t_ref)
    lane = lax.broadcasted_iota(jnp.int32, (8, LANES), 1)
    pos = ((dev * COLS + lane).astype(jnp.float32) * (1.0 / (16 * COLS)))[0:1, :]

    loads[0].wait()
    loads[1].wait()
    u = jnp.dot(xv[...], wv[...], preferred_element_type=jnp.float32)
    inv = 1.0 / jnp.sqrt(jnp.sum(u * u, axis=1, keepdims=True))
    q0[0] = (u * inv).astype(jnp.bfloat16)
    pl.semaphore_wait(barrier, 15)

    def pair_copy(slot):
        return pltpu.make_async_remote_copy(
            src_ref=q0.at[slot], dst_ref=q1.at[slot], send_sem=pair_s.at[slot], recv_sem=pair_r.at[slot],
            device_id=(relative(dev, 0, 1),), device_id_type=MESH)

    def link_copy(slot, src_slot, k):
        d = {1: k, 2: k + 1, 3: k + 2, 4: k + 1, 5: k + 2, 6: k + 2, 7: k + 2}[slot] % 3
        rows = pl.ds(OFF[k], LEN[k])
        return pltpu.make_async_remote_copy(
            src_ref=q0.at[src_slot, rows], dst_ref=q0.at[slot, rows],
            send_sem=link_s.at[slot * 3 + k], recv_sem=link_r.at[slot * 3 + k],
            device_id=(relative(dev, 1 << d, 0),), device_id_type=MESH)

    def wait_link(slot):
        for k in range(3):
            rows = pl.ds(OFF[k], LEN[k])
            pltpu.make_async_remote_copy(
                src_ref=q0.at[slot, rows], dst_ref=q0.at[slot, rows],
                send_sem=link_s.at[slot * 3 + k], recv_sem=link_r.at[slot * 3 + k],
                device_id=(relative(dev, 0, 1),), device_id_type=MESH).wait_recv()

    for slot in (1, 2, 3):
        for k in range(3):
            link_copy(slot, 0, k).start()
    pair_copy(0).start()
    loads[2].wait()

    def body(mm, ex, st):
        for i in range(4):
            if mm is not None:
                slot, h = mm
                s = lax.dot_general(q[h][slot], gv[512 * i:512 * (i + 1), :], (((1,), (1,)), ((), ())),
                                    preferred_element_type=jnp.float32)
                e[h][slot, :, 512 * i:512 * (i + 1)] = s
                m = jnp.maximum(jnp.maximum(s[:, 0:128], s[:, 128:256]), jnp.maximum(s[:, 256:384], s[:, 384:512]))
                ml[h][slot] = m if i == 0 else jnp.maximum(ml[h][slot], m)
            if ex is not None:
                slot, h = ex
                rows = slice(64 * i, 64 * (i + 1))
                m = ml[h][slot, rows, :]
                total = jnp.zeros((64, LANES), jnp.float32)
                ranked = jnp.zeros((64, LANES), jnp.float32)
                for j in reversed(range(TILES)):
                    cols = slice(LANES * j, LANES * (j + 1))
                    v = jnp.exp2((e[h][slot, rows, cols] - m) * cc)
                    e[h][slot, rows, cols] = v
                    ranked = ranked + total
                    total = total + v
                s_acc[h, rows, :] = total
                r_acc[h, rows, :] = ranked * (1.0 / (16 * TILES)) + total * pos
        if st is not None:
            slot, h = st
            for half in range(2):
                rows = slice(128 * half, 128 * (half + 1))
                mt = ml[h][slot, rows, :].T
                top = jnp.max(mt, axis=0, keepdims=True)
                w = jnp.exp2((mt - top) * cc)
                cst[slot, h, half:half + 1, :] = top
                cst[slot, h, 2 + half:3 + half, :] = jnp.sum(s_acc[h, rows, :].T * w, axis=0, keepdims=True)
                cst[slot, h, 4 + half:5 + half, :] = jnp.sum(r_acc[h, rows, :].T * w, axis=0, keepdims=True)

    body((0, 0), None, None)
    pair_copy(0).wait_recv()
    body((0, 1), (0, 0), None)

    def step(t, carry):
        wait_link_dyn(t)
        pair_dyn(t).start()

        @pl.when(t == 1)
        def _():
            for slot in (4, 5):
                for k in range(3):
                    link_copy(slot, 1, k).start()

        @pl.when(t == 2)
        def _():
            for k in range(3):
                link_copy(6, 2, k).start()

        @pl.when(t == 4)
        def _():
            for k in range(3):
                link_copy(7, 4, k).start()

        body((t, 0), (t - 1, 1), (t - 1, 0))
        pair_dyn(t).wait_recv()
        body((t, 1), (t, 0), (t - 1, 1))
        return carry

    wait_link_dyn, pair_dyn = wait_link, pair_copy
    lax.fori_loop(1, 8, step, 0)

    row = lax.broadcasted_iota(jnp.int32, (8, LANES), 0)
    lane8 = lax.broadcasted_iota(jnp.int32, (8, LANES), 1)
    query = (row % 2) * LANES + lane8
    first, second = query < OFF[1], query < OFF[2]

    def st_copy(v, h):
        i = 2 * (v ^ 7) + h
        return pltpu.make_async_remote_copy(
            src_ref=snd.at[i], dst_ref=rst.at[i], send_sem=st_s.at[i], recv_sem=st_r.at[i],
            device_id=(relative(dev, v ^ 7, h),), device_id_type=MESH)

    for v in range(7):
        for h in range(2):
            tiles = [cst[slot_of(v, k), h] for k in range(3)]
            snd[2 * (v ^ 7) + h] = jnp.where(first, tiles[0], jnp.where(second, tiles[1], tiles[2]))
    for v in range(7):
        for h in range(2):
            st_copy(v, h).start()

    body(None, (7, 1), (7, 0))
    body(None, None, (7, 1))
    snd[1] = cst[7, 1]
    st_copy(7, 1).start()

    def fb_copy(v, h):
        i = 2 * (v ^ 7) + h
        return pltpu.make_async_remote_copy(
            src_ref=mine, dst_ref=fin.at[i], send_sem=fb_s.at[i], recv_sem=fb_r.at[i],
            device_id=(relative(dev, v, h),), device_id_type=MESH)

    for v in range(8):
        for h in range(2):
            if v ^ 7 or h:
                st_copy(v, h).wait_recv()
    parts = [cst[7, 0]] + [rst[i] for i in range(1, 16)]
    top = functools.reduce(jnp.maximum, [part[0:2] for part in parts])
    total = jnp.zeros((2, LANES), jnp.float32)
    ranked = jnp.zeros((2, LANES), jnp.float32)
    for part in parts:
        w = jnp.exp2((part[0:2] - top) * cc)
        total = total + part[2:4] * w
        ranked = ranked + part[4:6] * w
    scale = 1.0 / total
    mine[0:2, :] = top
    mine[2:4, :] = scale
    mine[4:6, :] = ranked * scale
    mine[6:8, :] = jnp.zeros((2, LANES), jnp.float32)
    for v in range(8):
        for h in range(2):
            if v or h:
                fb_copy(v, h).start()
    fin[14] = mine[...]
    for v in range(8):
        for h in range(2):
            if v or h:
                fb_copy(v, h).wait_recv()
    for slot in range(8):
        for h in range(2):
            tiles = [fin[2 * source_mask(slot, k) + h] for k in range(3)]
            fin_out[slot, h] = jnp.where(first, tiles[0], jnp.where(second, tiles[1], tiles[2]))
    rank_out[...] = fin[...]

    for slot in range(8):
        pair_copy(slot).wait_send()
    for slot, src in ((1, 0), (2, 0), (3, 0), (4, 1), (5, 1), (6, 2), (7, 4)):
        for k in range(3):
            link_copy(slot, src, k).wait_send()
    for v in range(8):
        for h in range(2):
            if v ^ 7 or h:
                st_copy(v, h).wait_send()
            if v or h:
                fb_copy(v, h).wait_send()


NBUF = 3


def write_kernel(t_ref, e0, e1, ml0, ml1, fin, rank, p_hbm, r_out, stage, fac, sems):
    dev = lax.axis_index("ga")
    cc = scale_row(t_ref)
    for v in range(8):
        for h in range(2):
            r_out[pl.ds(2 * relative(dev, v, h), 2), :] = rank[2 * v + h, 4:6, :]

    def out_copy(slot, h, k, buf):
        v = jnp.int32(source_mask(0, k))
        for s in range(1, 8):
            v = jnp.where(slot == s, source_mask(s, k), v)
        src = dev
        for i, weight in ((0, 2), (1, 4), (2, 8)):
            src = src + (v // (1 << i)) % 2 * weight * (1 - 2 * ((dev // weight) % 2))
        if h:
            src = src + (1 - 2 * (dev % 2))
        row = pl.multiple_of(src * ROWS + OFF[k], 16)
        return pltpu.make_async_copy(stage.at[buf, pl.ds(OFF[k], LEN[k])], p_hbm.at[pl.ds(row, LEN[k])], sems.at[buf, k])

    def do_block(slot, h, n):
        buf = lax.rem(n, NBUF)

        @pl.when(n >= NBUF)
        def _():
            for k in range(3):
                out_copy(0, 0, k, buf).wait()

        eb, mb = (e0, e1)[h], (ml0, ml1)[h]
        for half in range(2):
            rows = slice(128 * half, 128 * (half + 1))
            top = jnp.broadcast_to(fin[slot, h, half:half + 1, :], (LANES, LANES)).T
            inv = jnp.broadcast_to(fin[slot, h, 2 + half:3 + half, :], (LANES, LANES)).T
            fac[rows, :] = jnp.exp2((mb[slot, rows, :] - top) * cc) * inv

        for k in range(3):
            for r in range(OFF[k], OFF[k] + LEN[k], 16):
                f = fac[r:r + 16, :]
                for j in range(TILES):
                    cols = slice(LANES * j, LANES * (j + 1))
                    stage[buf, r:r + 16, cols] = (eb[slot, r:r + 16, cols] * f).astype(jnp.bfloat16)
            out_copy(slot, h, k, buf).start()

    def step(t, carry):
        do_block(t, 0, 2 * t)
        do_block(t, 1, 2 * t + 1)
        return carry

    lax.fori_loop(0, 8, step, 0)
    for n in range(16 - NBUF, 16):
        for k in range(3):
            out_copy(0, 0, k, n % NBUF).wait()


def solution(mesh):
    vmem = pl.BlockSpec(memory_space=pltpu.VMEM)
    hbm = pl.BlockSpec(memory_space=pl.ANY)
    smem = pl.BlockSpec(memory_space=pltpu.SMEM)
    f32, bf16 = jnp.float32, jnp.bfloat16

    def per_device(text_states, text_proj, gallery, logit_scale):
        e0, e1, ml0, ml1, fin, rank = pl.pallas_call(
            score_kernel,
            out_shape=(
                pltpu.VMEM((8, ROWS, COLS), f32), pltpu.VMEM((8, ROWS, COLS), f32),
                pltpu.VMEM((8, ROWS, LANES), f32), pltpu.VMEM((8, ROWS, LANES), f32),
                pltpu.VMEM((8, 2, 8, LANES), f32), pltpu.VMEM((16, 8, LANES), f32),
            ),
            in_specs=[smem, hbm, hbm, hbm],
            out_specs=(vmem,) * 6,
            scratch_shapes=[
                pltpu.VMEM((ROWS, EMB), bf16), pltpu.VMEM((EMB, EMB), bf16), pltpu.VMEM((COLS, EMB), bf16),
                pltpu.VMEM((8, ROWS, EMB), bf16), pltpu.VMEM((8, ROWS, EMB), bf16),
                pltpu.VMEM((2, ROWS, LANES), f32), pltpu.VMEM((2, ROWS, LANES), f32),
                pltpu.VMEM((8, 2, 8, LANES), f32), pltpu.VMEM((16, 8, LANES), f32), pltpu.VMEM((16, 8, LANES), f32),
                pltpu.VMEM((8, LANES), f32), pltpu.VMEM((16, 8, LANES), f32),
                pltpu.SemaphoreType.DMA((3,)), pltpu.SemaphoreType.DMA((8,)), pltpu.SemaphoreType.DMA((8,)),
                pltpu.SemaphoreType.DMA((24,)), pltpu.SemaphoreType.DMA((24,)),
                pltpu.SemaphoreType.DMA((16,)), pltpu.SemaphoreType.DMA((16,)),
                pltpu.SemaphoreType.DMA((16,)), pltpu.SemaphoreType.DMA((16,)),
            ],
            compiler_params=pltpu.CompilerParams(collective_id=0, has_side_effects=True,
                                                 vmem_limit_bytes=26 * 1024 * 1024),
            name="score",
        )(logit_scale, text_states, text_proj, gallery)
        e0, e1, ml0, ml1, fin, rank = (pltpu.with_memory_space_constraint(a, pltpu.VMEM)
                                       for a in (e0, e1, ml0, ml1, fin, rank))
        prob, ranks = pl.pallas_call(
            write_kernel,
            out_shape=(jax.ShapeDtypeStruct((16 * ROWS, COLS), bf16), jax.ShapeDtypeStruct((32, LANES), f32)),
            in_specs=[smem] + [vmem] * 6,
            out_specs=(hbm, vmem),
            scratch_shapes=[pltpu.VMEM((NBUF, ROWS, COLS), bf16), pltpu.VMEM((ROWS, LANES), f32),
                            pltpu.SemaphoreType.DMA((NBUF, 3))],
            compiler_params=pltpu.CompilerParams(vmem_limit_bytes=26 * 1024 * 1024),
            name="write",
        )(logit_scale, e0, e1, ml0, ml1, fin, rank)
        return prob, ranks.reshape(32 * LANES)

    return jax.shard_map(per_device, mesh=mesh,
                         in_specs=(P("ga", None), P(None, None), P("ga", None), P(None)),
                         out_specs=(P(None, "ga"), P(None)), check_vma=False)
```
